32 devices in a mesh: grp: 8 (over z, core), sib: 4 (over y, x).
Axes of the slice: x: 2, y: 2, z: 4, core: 2. Of those that a mesh axis runs over, the one named last changes fastest.
Arguments:
- targets: float32 [40960, 256], P(('grp', 'sib')), may hold values from -6 to 6
- leaf_order: int32 [32, 1280], P(('grp', 'sib')), may hold values from 0 to 1279, each once within a row
- near_block: float32 [40960, 1280], P(('grp', 'sib')), may hold values from -0.15625 to 0.15625
- leaf_basis: float32 [40960, 128], P(('grp', 'sib')), may hold values from -0.15625 to 0.15625
- sibling_coupling: float32 [4096, 512], P(('grp', 'sib')), may hold values from -0.5 to 0.5
- transfer: float32 [4096, 128], P(('grp', 'sib')), may hold values from -0.5 to 0.5
- top_coupling: float32 [1024, 1024], P('grp', 'sib'), may hold values from -0.1875 to 0.1875
Outputs:
- coefficients: float32 [40960, 256], P(('grp', 'sib'))
- fitted: float32 [40960, 256], P(('grp', 'sib'))
The draws below stay inside these ranges and needn't reach their ends.
Inputs may be any that keep to these rules, and one draw needn't show every extreme that they name: `leaf_order`: each row of 1280 entries holds every number of 0 to 1279 once.
All inputs are finite; a program needn't handle non-finite values.
Results may differ from the reference program's by a relative error of at most 0.00025.
Values sent between devices are 32-bit elements; how exact they have to be, the bound alone decides.
A program may use at most 64 MiB of HBM per device.

```python
import jax
import jax.numpy as jnp
from jax import lax

LEAF = 1280
COUPLING_RANK = 128
TARGET_COLUMNS = 256
ITERS = 3
POINTS = 40960
N_GRP = 8
N_SIB = 4
DEVICES = 32


def level_of(own_key, shape, cuts, smallest, high):
    def one(dim, parts):
        draws = jax.random.uniform(jax.random.fold_in(jax.random.fold_in(own_key, 6), dim), (parts,), jnp.float32, smallest / len(cuts), high / len(cuts))
        return jnp.repeat(jnp.exp(draws), shape[dim] // parts).reshape((-1,) + (1,) * (len(shape) - dim - 1))

    factor_of = one(*cuts[0])
    for cut in cuts[1:]:
        factor_of = factor_of * one(*cut)
    return factor_of


def gaussian(own_key, dims, scale, bound, pieces=(), held_as=jnp.bfloat16):
    drawn = jax.random.normal(own_key, dims, jnp.float32) * scale
    if len(pieces) > 0:
        drawn = level_of(own_key, dims, pieces, -0.22, 0.18) * drawn
    return jnp.clip(drawn, min=-bound, max=bound).astype(held_as)


def setup_inputs(seed: int = 0) -> dict:
    arg_keys = jax.random.split(jax.random.key(seed), 8)
    return {
        "targets": gaussian(arg_keys[0], (POINTS, TARGET_COLUMNS), 1.0, 6.0, ((0, 32),), jnp.float32),
        "leaf_order": jax.vmap(lambda own: jax.random.permutation(own, LEAF))(jax.random.split(arg_keys[1], DEVICES)).reshape((DEVICES, LEAF)).astype(jnp.int32),
        "near_block": gaussian(arg_keys[2], (POINTS, LEAF), LEAF ** -0.5, 0.15625, ((0, 32),), jnp.float32),
        "leaf_basis": gaussian(arg_keys[3], (POINTS, COUPLING_RANK), LEAF ** -0.5, 0.15625, ((0, 32),), jnp.float32),
        "sibling_coupling": gaussian(arg_keys[4], (DEVICES * COUPLING_RANK, N_SIB * COUPLING_RANK), COUPLING_RANK ** -0.5, 0.5, ((0, 32),), jnp.float32),
        "transfer": gaussian(arg_keys[5], (DEVICES * COUPLING_RANK, COUPLING_RANK), COUPLING_RANK ** -0.5, 0.5, ((0, 32),), jnp.float32),
        "top_coupling": gaussian(arg_keys[6], (N_GRP * COUPLING_RANK, N_GRP * COUPLING_RANK), (N_GRP * COUPLING_RANK) ** -0.5, 0.1875, ((0, 8), (1, 4)), jnp.float32),
    }


step_size = 0.5
shrink_rate = 0.1
highest_level = lax.Precision.HIGHEST


def reference(targets, leaf_order, near_block, leaf_basis, sibling_coupling, transfer, top_coupling):
    ordering = leaf_order.reshape(DEVICES, LEAF).astype(jnp.int32)
    leaf_targets = targets.reshape(DEVICES, LEAF, TARGET_COLUMNS)
    tree_targets = jnp.take_along_axis(leaf_targets, ordering[:, :, None], axis=1)
    nearby_blocks = near_block.reshape(DEVICES, LEAF, LEAF)
    nested_basis = leaf_basis.reshape(DEVICES, LEAF, COUPLING_RANK)
    sib_mask = 1.0 - jnp.eye(N_SIB, dtype=jnp.float32)
    sibling = sibling_coupling.reshape(N_GRP, N_SIB, COUPLING_RANK, N_SIB, COUPLING_RANK) * sib_mask[None, :, None, :, None]
    upward_pass = transfer.reshape(N_GRP, N_SIB, COUPLING_RANK, COUPLING_RANK)
    grp_mask = 1.0 - jnp.eye(N_GRP, dtype=jnp.float32)
    root_level = top_coupling.reshape(N_GRP, COUPLING_RANK, N_GRP, COUPLING_RANK) * grp_mask[:, None, :, None]

    def apply_kernel(weight_coefficients):
        nearby_part = jnp.einsum('yac,ycf->yaf', nearby_blocks, weight_coefficients, precision=highest_level)
        leaf_coefficients = jnp.einsum('ojq,ojv->oqv', nested_basis, weight_coefficients, precision=highest_level).reshape(N_GRP, N_SIB, COUPLING_RANK, TARGET_COLUMNS)
        sibling_sum = jnp.einsum('gsrkq,gkqt->gsrt', sibling, leaf_coefficients, precision=highest_level)
        cluster_coefficient = jnp.einsum('cyma,cymd->cad', upward_pass, leaf_coefficients, precision=highest_level)
        root_sum = jnp.einsum('pizc,zce->pie', root_level, cluster_coefficient, precision=highest_level)
        downward_pass = sibling_sum + jnp.einsum('gsrq,gqt->gsrt', upward_pass, root_sum, precision=highest_level)
        distant_part = jnp.einsum('lsy,lyj->lsj', nested_basis, downward_pass.reshape(DEVICES, COUPLING_RANK, TARGET_COLUMNS), precision=highest_level)
        return nearby_part + distant_part

    weight_coefficients = step_size * tree_targets
    fitted = weight_coefficients
    for iteration in range(ITERS):
        fitted = jnp.tanh(apply_kernel(weight_coefficients))
        weight_coefficients = weight_coefficients + step_size * (tree_targets - fitted) - step_size * shrink_rate * weight_coefficients
    leaves = jnp.arange(DEVICES).astype(jnp.int32)[:, None]
    coeffs_out = jnp.zeros_like(weight_coefficients).at[leaves, ordering].set(weight_coefficients)
    fitted_out = jnp.zeros_like(fitted).at[leaves, ordering].set(fitted)
    return coeffs_out.reshape(POINTS, TARGET_COLUMNS), fitted_out.reshape(POINTS, TARGET_COLUMNS)
```

```python
import functools

import jax
import jax.numpy as jnp
from jax import lax
from jax.experimental import pallas as pl
from jax.experimental.pallas import tpu as pltpu
from jax.sharding import PartitionSpec as P

ITERS = 3
step_size = 0.5
shrink_rate = 0.1
f32 = jnp.float32
bf16 = jnp.bfloat16
MESH = pl.DeviceIdType.MESH


def split(value):
    high = value.astype(bf16)
    return high, (value - high.astype(f32)).astype(bf16)


def dot(left, right):
    return jnp.dot(left, right, preferred_element_type=f32)


def dot3(left, right):
    return dot(left[0], right[0]) + (dot(left[0], right[1]) + dot(left[1], right[0]))


def kernel(n_grp, n_sib, targets, order, near, basis, sibling, transfer, top,
           prev_out, field_out,
           t_v, o_v, n_v, u_v, s_v, r_v, top_v,
           oc_v, g_v, gt_v, nh_v, nl_v, uh_v, ul_v, wh_v, wl_v, ph_v, pl_v,
           uwh_v, uwl_v, bh_v, bl_v, tt_v, x_v, xh_v, xl_v, pre_v, prev_v,
           c_own, c_all, d_own, d_sib, d_grp, z_all,
           load_sem, out_sem, top_send, top_recv, d_send, d_recv, c_send, c_recv,
           g_send, g_recv, z_send, z_recv):
    leaf, cols = t_v.shape
    rank = r_v.shape[0]
    part = cols // n_sib
    tile = 256 if leaf % 256 == 0 else leaf
    tiles = leaf // tile
    n_chip = n_grp // 2
    grp, sib = lax.axis_index("grp"), lax.axis_index("sib")
    chip, core = lax.div(grp, 2), lax.rem(grp, 2)
    partner = (grp + 1 - 2 * core, sib)

    def sib_at(k):
        return lax.rem(sib + k + n_sib, n_sib)

    def chip_at(k):
        return lax.rem(chip + k + n_chip, n_chip)

    peers = [(grp, sib_at(k)) for k in range(1, n_sib)]
    peers += [(chip_at(k) * 2 + core, sib) for k in range(1, n_chip)] + [partner]
    barrier = pltpu.get_barrier_semaphore()
    for peer in peers:
        pl.semaphore_signal(barrier, inc=1, device_id=peer, device_id_type=MESH)

    loads = [pltpu.make_async_copy(src, dst, load_sem.at[i]) for i, (src, dst) in enumerate((
        (order, o_v), (targets, t_v), (basis, u_v), (transfer, r_v), (near, n_v),
        (sibling, s_v), (top, top_v.at[sib])))]
    for load in loads:
        load.start()
    pending = []

    def send(src, dst, send_sem, recv_sem, peer):
        copy = pltpu.make_async_remote_copy(
            src_ref=src, dst_ref=dst, send_sem=send_sem, recv_sem=recv_sem,
            device_id=peer, device_id_type=MESH)
        copy.start()
        pending.append(copy)
        return copy

    def rows(i):
        return pl.ds(pl.multiple_of(i * tile, tile), tile)

    def over_tiles(first, last, body):
        if last > first:
            pl.loop(first, last)(lambda i: body(rows(i), i))

    loads[0].wait()
    oc_v[...] = jnp.broadcast_to(o_v[...].astype(f32), (128, leaf)).T
    pl.semaphore_wait(barrier, len(peers))
    top_copies = [send(top, top_v.at[sib], top_send.at[k], top_recv.at[k], (grp, sib_at(k)))
                  for k in range(1, n_sib)]
    loads[1].wait()
    loads[2].wait()
    loads[3].wait()

    th, tl = split(t_v[...])
    xh_v[...] = th
    tlow = tl
    prev_v[...] = jnp.zeros_like(prev_v)
    xl_v[...] = tlow

    def to_tree(r, i):
        own = oc_v[r, :]
        for b in range(leaf // 128):
            hit = own == (lax.broadcasted_iota(jnp.int32, (tile, 128), 1) + 128 * b).astype(f32)
            g_v[:, b * 128:(b + 1) * 128] = jnp.where(hit, 1.0, 0.0).astype(bf16)
        tt_v[r, :] = dot(g_v[...], xh_v[...]) + dot(g_v[...], xl_v[...])

    over_tiles(0, tiles, to_tree)

    def start_x(r, i):
        value = step_size * tt_v[r, :]
        x_v[r, :] = value
        xh_v[r, :], xl_v[r, :] = split(value)

    over_tiles(0, tiles, start_x)

    r_pair = split(r_v[...])
    ut = u_v[...].T
    ut_pair = split(ut)
    uwh_v[:rank, :], uwl_v[:rank, :] = ut_pair
    uwh_v[rank:, :], uwl_v[rank:, :] = split(dot3(split(r_v[...].T), ut_pair))

    def second_basis(r, i):
        pair = split(u_v[r, :])
        uh_v[r, :], ul_v[r, :] = pair
        wh_v[r, :], wl_v[r, :] = split(dot3(pair, r_pair))

    def near_first(r, i):
        pair = split(n_v[r, :])
        nh_v[r, :], nl_v[r, :] = pair
        pre_v[r, :] = dot3(pair, (xh_v[...], xl_v[...]))

    def near_again(r, i):
        pre_v[r, :] = dot3((nh_v[r, :], nl_v[r, :]), (xh_v[...], xl_v[...]))

    def to_data(r, i):
        q = lax.broadcasted_iota(jnp.int32, (tile, leaf), 0) + i * tile
        gt_v[r, :] = jnp.where(q == o_v[...], 1.0, 0.0).astype(bf16)
        ph_v[r, :] = dot(gt_v[r, :], wh_v[...]).astype(bf16)
        pl_v[r, :] = dot(gt_v[r, :], wl_v[...]).astype(bf16)

    for it in range(ITERS):
        final = it == ITERS - 1
        both = dot3((uwh_v[...], uwl_v[...]), (xh_v[...], xl_v[...]))
        d_own[it] = both[rank:, :].T
        d_copies = [send(d_own.at[it, pl.ds(pl.multiple_of(sib_at(k) * part, part), part)], d_sib.at[it, k],
                         d_send.at[it, k], d_recv.at[it, k], (grp, sib_at(k))) for k in range(1, n_sib)]
        c_own[it] = both[:rank, :]
        c_copies = [send(c_own.at[it], c_all.at[it, k], c_send.at[it, k], c_recv.at[it, k],
                         (grp, sib_at(k))) for k in range(1, n_sib)]
        if it == 0:
            over_tiles(0, tiles, second_basis)
            loads[4].wait()
        near_part = near_first if it == 0 else near_again
        early = (tiles + 1) // 2 if it == 0 else tiles
        over_tiles(0, early, near_part)

        total = d_own[it, pl.ds(pl.multiple_of(sib * part, part), part), :]
        for k in range(1, n_sib):
            d_copies[k - 1].wait_recv()
            total = total + d_sib[it, k]
        d_grp[it, 0, 0] = total
        mine = d_grp.at[it, 0, 0]
        g_copies = [send(mine, d_grp.at[it, k, 0], g_send.at[it, k, 0], g_recv.at[it, k, 0],
                         (chip_at(k) * 2 + core, sib)) for k in range(1, n_chip)]
        relays = [send(mine, d_grp.at[it, 0, 1], g_send.at[it, 0, 1], g_recv.at[it, 0, 1], partner)]

        over_tiles(early, tiles, near_part)
        if it == 0:
            for copy in top_copies:
                copy.wait_recv()
            loads[5].wait()
            loads[6].wait()
            width = top_v.shape[2]
            for j in range(n_sib):
                bh_v[j * width:(j + 1) * width, :], bl_v[j * width:(j + 1) * width, :] = split(top_v[j].T)
            over_tiles(0, tiles, to_data)
        if final:
            def prev_to_data(r, i):
                prev_v[r, :] = dot(gt_v[r, :], xh_v[...]) + dot(gt_v[r, :], xl_v[...])
            over_tiles(0, tiles, prev_to_data)
            out_prev = pltpu.make_async_copy(prev_v, prev_out, out_sem.at[0])
            out_prev.start()

        def from_group(k, other):
            group = chip_at(-k) * 2 + (1 - core if other else core)
            at = pl.ds(pl.multiple_of(group * rank, rank), rank)
            return dot3(split(d_grp[it, k, other]), (bh_v[at, :], bl_v[at, :]))

        for k in range(1, n_chip):
            g_copies[k - 1].wait_recv()
            relays.append(send(d_grp.at[it, k, 0], d_grp.at[it, k, 1], g_send.at[it, k, 1],
                               g_recv.at[it, k, 1], partner))
        relays[0].wait_recv()
        z_part = from_group(0, 1)
        for k in range(1, n_chip):
            z_part = z_part + from_group(k, 0)
        for k in range(1, n_chip):
            relays[k].wait_recv()
            z_part = z_part + from_group(k, 1)
        here = pl.ds(pl.multiple_of(sib * part, part), part)
        z_all[it, here, :] = z_part
        z_copies = [send(z_all.at[it, here], z_all.at[it, here], z_send.at[it, k], z_recv.at[it, k],
                         (grp, sib_at(k))) for k in range(1, n_sib)]

        down = jnp.zeros((rank, cols), f32)
        for k in range(1, n_sib):
            c_copies[k - 1].wait_recv()
            block = s_v[:, pl.ds(pl.multiple_of(sib_at(-k) * rank, rank), rank)]
            down = down + dot3(split(block), split(c_all[it, k]))
        down_pair = split(down)

        def add_siblings(r, i):
            pre_v[r, :] = pre_v[r, :] + dot3((uh_v[r, :], ul_v[r, :]), down_pair)

        over_tiles(0, tiles, add_siblings)
        if final:
            def pre_split(r, i):
                xh_v[r, :], xl_v[r, :] = split(pre_v[r, :])

            def pre_to_data(r, i):
                pre_v[r, :] = dot(gt_v[r, :], xh_v[...]) + dot(gt_v[r, :], xl_v[...])

            over_tiles(0, tiles, pre_split)
            over_tiles(0, tiles, pre_to_data)

        for copy in z_copies:
            copy.wait_recv()
        z_pair = split(z_all[it].T)
        if final:
            outs = []
            for i in range(tiles):
                r = pl.ds(i * tile, tile)
                pre_v[r, :] = pre_v[r, :] + dot3((ph_v[r, :], pl_v[r, :]), z_pair)
                outs.append(pltpu.make_async_copy(pre_v.at[r], field_out.at[r], out_sem.at[1 + i]))
                outs[-1].start()
        else:
            def update(r, i):
                fitted = jnp.tanh(pre_v[r, :] + dot3((wh_v[r, :], wl_v[r, :]), z_pair))
                old = x_v[r, :]
                new = old + step_size * (tt_v[r, :] - fitted) - step_size * shrink_rate * old
                x_v[r, :] = new
                xh_v[r, :], xl_v[r, :] = split(new)

            over_tiles(0, tiles, update)

    for copy in pending:
        copy.wait_send()
    out_prev.wait()
    for copy in outs:
        copy.wait()


def shards(n_grp, n_sib, targets, leaf_order, near_block, leaf_basis, sibling_coupling, transfer, top_coupling):
    leaf, cols = targets.shape
    rank = transfer.shape[0]
    part = cols // n_sib
    tile = 256 if leaf % 256 == 0 else leaf
    n_chip = n_grp // 2
    dma = pltpu.SemaphoreType.DMA
    vmem = pltpu.VMEM
    previous, field = pl.pallas_call(
        functools.partial(kernel, n_grp, n_sib),
        out_shape=(jax.ShapeDtypeStruct((leaf, cols), f32),) * 2,
        in_specs=[pl.BlockSpec(memory_space=pl.ANY)] * 7,
        out_specs=(pl.BlockSpec(memory_space=pl.ANY),) * 2,
        scratch_shapes=[
            vmem((leaf, cols), f32), vmem((1, leaf), jnp.int32), vmem((leaf, leaf), f32),
            vmem((leaf, rank), f32), vmem(sibling_coupling.shape, f32), vmem((rank, rank), f32),
            vmem((n_sib,) + top_coupling.shape, f32),
            vmem((leaf, 128), f32), vmem((tile, leaf), bf16), vmem((leaf, leaf), bf16),
            vmem((leaf, leaf), bf16), vmem((leaf, leaf), bf16)]
        + [vmem((leaf, rank), bf16)] * 6
        + [vmem((2 * rank, leaf), bf16)] * 2
        + [vmem((n_grp * rank, rank), bf16)] * 2
        + [vmem((leaf, cols), f32)] * 2 + [vmem((leaf, cols), bf16)] * 2 + [vmem((leaf, cols), f32)] * 2
        + [
            vmem((ITERS, rank, cols), f32), vmem((ITERS, n_sib, rank, cols), f32),
            vmem((ITERS, cols, rank), f32), vmem((ITERS, n_sib, part, rank), f32),
            vmem((ITERS, n_chip, 2, part, rank), f32), vmem((ITERS, cols, rank), f32),
            dma((7,)), dma((1 + leaf // tile,)), dma((n_sib,)), dma((n_sib,)),
            dma((ITERS, n_sib)), dma((ITERS, n_sib)), dma((ITERS, n_sib)), dma((ITERS, n_sib)),
            dma((ITERS, n_chip, 2)), dma((ITERS, n_chip, 2)), dma((ITERS, n_sib)), dma((ITERS, n_sib))],
        compiler_params=pltpu.CompilerParams(
            collective_id=0, has_side_effects=True, vmem_limit_bytes=56 * 1024 * 1024),
    )(targets, leaf_order, near_block, leaf_basis, sibling_coupling, transfer, top_coupling)
    fitted = jnp.tanh(field)
    coefficients = previous + step_size * (targets - fitted) - step_size * shrink_rate * previous
    return coefficients, fitted


def solution(mesh):
    spec = P(("grp", "sib"), None)
    return jax.shard_map(
        functools.partial(shards, mesh.shape["grp"], mesh.shape["sib"]),
        mesh=mesh,
        in_specs=(spec,) * 6 + (P("grp", "sib"),),
        out_specs=(spec, spec),
        check_vma=False,
    )
```

```python
import functools

import jax
import jax.numpy as jnp
from jax import lax
from jax.experimental import pallas as pl
from jax.experimental.pallas import tpu as pltpu
from jax.sharding import PartitionSpec as P

ITERS = 3
step_size = 0.5
shrink_rate = 0.1
f32 = jnp.float32
bf16 = jnp.bfloat16
MESH = pl.DeviceIdType.MESH


def split(value):
    high = value.astype(bf16)
    return high, (value - high.astype(f32)).astype(bf16)


def dot(left, right):
    return jnp.dot(left, right, preferred_element_type=f32)


def dot3(left, right):
    return dot(left[0], right[0]) + (dot(left[0], right[1]) + dot(left[1], right[0]))


def kernel(n_grp, n_sib, targets, order, near, basis, sibling, transfer, top,
           prev_out, field_out,
           t_v, o_v, n_v, u_v, s_v, r_v, top_v,
           oc_v, g_v, gt_v, nh_v, nl_v, b_v, p_v,
           uwh_v, uwl_v, bh_v, bl_v, tt_v, x_v, xh_v, xl_v, pre_v, prev_v,
           c_own, c_all, d_own, d_sib, d_grp, z_all,
           load_sem, out_sem, top_send, top_recv, d_send, d_recv, c_send, c_recv,
           g_send, g_recv, z_send, z_recv):
    leaf, cols = t_v.shape
    rank = r_v.shape[0]
    part = cols // n_sib
    tile = 256 if leaf % 256 == 0 else leaf
    tiles = leaf // tile
    n_chip = n_grp // 2
    grp, sib = lax.axis_index("grp"), lax.axis_index("sib")
    chip, core = lax.div(grp, 2), lax.rem(grp, 2)
    partner = (grp + 1 - 2 * core, sib)

    def sib_at(k):
        return lax.rem(sib + k + n_sib, n_sib)

    def chip_at(k):
        return lax.rem(chip + k + n_chip, n_chip)

    peers = [(grp, sib_at(k)) for k in range(1, n_sib)]
    peers += [(chip_at(k) * 2 + core, sib) for k in range(1, n_chip)] + [partner]
    barrier = pltpu.get_barrier_semaphore()
    for peer in peers:
        pl.semaphore_signal(barrier, inc=1, device_id=peer, device_id_type=MESH)

    loads = [pltpu.make_async_copy(src, dst, load_sem.at[i]) for i, (src, dst) in enumerate((
        (order, o_v), (targets, t_v), (basis, u_v), (transfer, r_v), (near, n_v),
        (sibling, s_v), (top, top_v.at[sib])))]
    for load in loads:
        load.start()
    pending = []

    def send(src, dst, send_sem, recv_sem, peer):
        copy = pltpu.make_async_remote_copy(
            src_ref=src, dst_ref=dst, send_sem=send_sem, recv_sem=recv_sem,
            device_id=peer, device_id_type=MESH)
        copy.start()
        pending.append(copy)
        return copy

    def rows(i):
        return pl.ds(pl.multiple_of(i * tile, tile), tile)

    def over_tiles(first, last, body):
        if last > first:
            pl.loop(first, last)(lambda i: body(rows(i), i))

    loads[0].wait()
    oc_v[...] = jnp.broadcast_to(o_v[...].astype(f32), (128, leaf)).T
    pl.semaphore_wait(barrier, len(peers))
    top_copies = [send(top, top_v.at[sib], top_send.at[k], top_recv.at[k], (grp, sib_at(k)))
                  for k in range(1, n_sib)]
    loads[1].wait()
    loads[2].wait()
    loads[3].wait()

    xh_v[...], xl_v[...] = split(t_v[...])

    def to_tree(r, i):
        own = oc_v[r, :]
        for b in range(leaf // 128):
            hit = own == (lax.broadcasted_iota(jnp.int32, (tile, 128), 1) + 128 * b).astype(f32)
            g_v[:, b * 128:(b + 1) * 128] = jnp.where(hit, 1.0, 0.0).astype(bf16)
        tt_v[r, :] = dot(g_v[...], xh_v[...]) + dot(g_v[...], xl_v[...])

    over_tiles(0, tiles, to_tree)

    def start_x(r, i):
        value = step_size * tt_v[r, :]
        x_v[r, :] = value
        xh_v[r, :], xl_v[r, :] = split(value)

    over_tiles(0, tiles, start_x)

    r_pair = split(r_v[...])
    ut = u_v[...].T
    ut_pair = split(ut)
    uwh_v[:rank, :], uwl_v[:rank, :] = ut_pair
    uwh_v[rank:, :], uwl_v[rank:, :] = split(dot3(split(r_v[...].T), ut_pair))

    def second_basis(r, i):
        pair = split(u_v[r, :])
        b_v[r, :rank], b_v[r, rank:2 * rank] = split(dot3(pair, r_pair))
        b_v[r, 2 * rank:3 * rank], b_v[r, 3 * rank:] = pair

    def times_basis(ref, r, at, pair, twice):
        return dot(ref[r, at:at + 2 * rank], twice) + dot(ref[r, at:at + rank], pair[1])

    def near_first(r, i):
        pair = split(n_v[r, :])
        nh_v[r, :], nl_v[r, :] = pair
        pre_v[r, :] = dot3(pair, (xh_v[...], xl_v[...]))

    def near_again(r, i):
        pre_v[r, :] = dot3((nh_v[r, :], nl_v[r, :]), (xh_v[...], xl_v[...]))

    def to_data(r, i):
        q = lax.broadcasted_iota(jnp.int32, (tile, leaf), 0) + i * tile
        gt_v[r, :] = jnp.where(q == o_v[...], 1.0, 0.0).astype(bf16)
        p_v[r, :] = dot(gt_v[r, :], b_v[...]).astype(bf16)

    for it in range(ITERS):
        final = it == ITERS - 1
        both = dot3((uwh_v[...], uwl_v[...]), (xh_v[...], xl_v[...]))
        d_own[it] = both[rank:, :].T
        d_copies = [send(d_own.at[it, pl.ds(pl.multiple_of(sib_at(k) * part, part), part)], d_sib.at[it, k],
                         d_send.at[it, k], d_recv.at[it, k], (grp, sib_at(k))) for k in range(1, n_sib)]
        c_own[it] = both[:rank, :]
        if it == 0:
            loads[4].wait()
        near_part = near_first if it == 0 else near_again
        early = (tiles + 1) // 2 if it == 0 else max(tiles - 1, 1)
        over_tiles(0, early, near_part)

        total = d_own[it, pl.ds(pl.multiple_of(sib * part, part), part), :]
        for k in range(1, n_sib):
            d_copies[k - 1].wait_recv()
            total = total + d_sib[it, k]
        d_grp[it, 0, 0] = total
        mine = d_grp.at[it, 0, 0]
        g_copies = [send(mine, d_grp.at[it, k, 0], g_send.at[it, k, 0], g_recv.at[it, k, 0],
                         (chip_at(k) * 2 + core, sib)) for k in range(1, n_chip)]
        relays = [send(mine, d_grp.at[it, 0, 1], g_send.at[it, 0, 1], g_recv.at[it, 0, 1], partner)]

        c_copies = [send(c_own.at[it], c_all.at[it, k], c_send.at[it, k], c_recv.at[it, k],
                         (grp, sib_at(k))) for k in range(1, n_sib)]

        over_tiles(early, tiles, near_part)
        if it == 0:
            over_tiles(0, tiles, second_basis)
            for copy in top_copies:
                copy.wait_recv()
            loads[5].wait()
            loads[6].wait()
            width = top_v.shape[2]
            for j in range(n_sib):
                bh_v[j * width:(j + 1) * width, :], bl_v[j * width:(j + 1) * width, :] = split(top_v[j].T)
            over_tiles(0, tiles, to_data)
        if final:
            def prev_to_data(r, i):
                prev_v[r, :] = dot(gt_v[r, :], xh_v[...]) + dot(gt_v[r, :], xl_v[...])
            over_tiles(0, tiles, prev_to_data)
            out_prev = pltpu.make_async_copy(prev_v, prev_out, out_sem.at[0])
            out_prev.start()

            def pre_split(r, i):
                xh_v[r, :], xl_v[r, :] = split(pre_v[r, :])

            def pre_to_data(r, i):
                pre_v[r, :] = dot(gt_v[r, :], xh_v[...]) + dot(gt_v[r, :], xl_v[...])

            over_tiles(0, tiles, pre_split)
            over_tiles(0, tiles, pre_to_data)

        def from_group(k, other):
            group = chip_at(-k) * 2 + (1 - core if other else core)
            at = pl.ds(pl.multiple_of(group * rank, rank), rank)
            return dot3(split(d_grp[it, k, other]), (bh_v[at, :], bl_v[at, :]))

        for k in range(1, n_chip):
            g_copies[k - 1].wait_recv()
            relays.append(send(d_grp.at[it, k, 0], d_grp.at[it, k, 1], g_send.at[it, k, 1],
                               g_recv.at[it, k, 1], partner))
        relays[0].wait_recv()
        z_part = from_group(0, 1)
        for k in range(1, n_chip):
            z_part = z_part + from_group(k, 0)
        for k in range(1, n_chip):
            relays[k].wait_recv()
            z_part = z_part + from_group(k, 1)
        here = pl.ds(pl.multiple_of(sib * part, part), part)
        z_all[it, here, :] = z_part
        z_copies = [send(z_all.at[it, here], z_all.at[it, here], z_send.at[it, k], z_recv.at[it, k],
                         (grp, sib_at(k))) for k in range(1, n_sib)]

        down = jnp.zeros((rank, cols), f32)
        for k in range(1, n_sib):
            c_copies[k - 1].wait_recv()
            block = s_v[:, pl.ds(pl.multiple_of(sib_at(-k) * rank, rank), rank)]
            down = down + dot3(split(block), split(c_all[it, k]))
        down_pair = split(down)
        down_twice = jnp.concatenate([down_pair[0]] * 2, axis=0)
        basis_v = p_v if final else b_v

        def add_siblings(r, i):
            pre_v[r, :] = pre_v[r, :] + times_basis(basis_v, r, 2 * rank, down_pair, down_twice)

        for i in range(tiles):
            add_siblings(pl.ds(i * tile, tile), i)

        for copy in z_copies:
            copy.wait_recv()
        z_pair = split(z_all[it].T)
        z_twice = jnp.concatenate([z_pair[0]] * 2, axis=0)
        if final:
            outs = []
            for i in range(tiles):
                r = pl.ds(i * tile, tile)
                pre_v[r, :] = pre_v[r, :] + times_basis(p_v, r, 0, z_pair, z_twice)
                outs.append(pltpu.make_async_copy(pre_v.at[r], field_out.at[r], out_sem.at[1 + i]))
                outs[-1].start()
        else:
            def update(r, i):
                fitted = jnp.tanh(pre_v[r, :] + times_basis(b_v, r, 0, z_pair, z_twice))
                old = x_v[r, :]
                new = old + step_size * (tt_v[r, :] - fitted) - step_size * shrink_rate * old
                x_v[r, :] = new
                xh_v[r, :], xl_v[r, :] = split(new)

            for i in range(tiles):
                update(pl.ds(i * tile, tile), i)

    for copy in pending:
        copy.wait_send()
    out_prev.wait()
    for copy in outs:
        copy.wait()


def shards(n_grp, n_sib, targets, leaf_order, near_block, leaf_basis, sibling_coupling, transfer, top_coupling):
    leaf, cols = targets.shape
    rank = transfer.shape[0]
    part = cols // n_sib
    tile = 256 if leaf % 256 == 0 else leaf
    n_chip = n_grp // 2
    dma = pltpu.SemaphoreType.DMA
    vmem = pltpu.VMEM
    previous, field = pl.pallas_call(
        functools.partial(kernel, n_grp, n_sib),
        out_shape=(jax.ShapeDtypeStruct((leaf, cols), f32),) * 2,
        in_specs=[pl.BlockSpec(memory_space=pl.ANY)] * 7,
        out_specs=(pl.BlockSpec(memory_space=pl.ANY),) * 2,
        scratch_shapes=[
            vmem((leaf, cols), f32), vmem((1, leaf), jnp.int32), vmem((leaf, leaf), f32),
            vmem((leaf, rank), f32), vmem(sibling_coupling.shape, f32), vmem((rank, rank), f32),
            vmem((n_sib,) + top_coupling.shape, f32),
            vmem((leaf, 128), f32), vmem((tile, leaf), bf16), vmem((leaf, leaf), bf16),
            vmem((leaf, leaf), bf16), vmem((leaf, leaf), bf16)]
        + [vmem((leaf, 4 * rank), bf16)] * 2
        + [vmem((2 * rank, leaf), bf16)] * 2
        + [vmem((n_grp * rank, rank), bf16)] * 2
        + [vmem((leaf, cols), f32)] * 2 + [vmem((leaf, cols), bf16)] * 2 + [vmem((leaf, cols), f32)] * 2
        + [
            vmem((ITERS, rank, cols), f32), vmem((ITERS, n_sib, rank, cols), f32),
            vmem((ITERS, cols, rank), f32), vmem((ITERS, n_sib, part, rank), f32),
            vmem((ITERS, n_chip, 2, part, rank), f32), vmem((ITERS, cols, rank), f32),
            dma((7,)), dma((1 + leaf // tile,)), dma((n_sib,)), dma((n_sib,)),
            dma((ITERS, n_sib)), dma((ITERS, n_sib)), dma((ITERS, n_sib)), dma((ITERS, n_sib)),
            dma((ITERS, n_chip, 2)), dma((ITERS, n_chip, 2)), dma((ITERS, n_sib)), dma((ITERS, n_sib))],
        compiler_params=pltpu.CompilerParams(
            collective_id=0, has_side_effects=True, vmem_limit_bytes=56 * 1024 * 1024),
    )(targets, leaf_order, near_block, leaf_basis, sibling_coupling, transfer, top_coupling)
    fitted = jnp.tanh(field)
    coefficients = previous + step_size * (targets - fitted) - step_size * shrink_rate * previous
    return coefficients, fitted


def solution(mesh):
    spec = P(("grp", "sib"), None)
    return jax.shard_map(
        functools.partial(shards, mesh.shape["grp"], mesh.shape["sib"]),
        mesh=mesh,
        in_specs=(spec,) * 6 + (P("grp", "sib"),),
        out_specs=(spec, spec),
        check_vma=False,
    )
```
